32 devices in a mesh: row: 4 (over z), col: 8 (over y, x, core).
Axes of the slice: x: 2, y: 2, z: 4, core: 2. Of those that a mesh axis runs over, the one named last changes fastest.
Arguments:
- a_matrix: float32 [16384, 16384], P('row', 'col'), may hold values from -2.25 to 2.25
- b_matrix: float32 [16384, 16384], P('row', 'col'), may hold values from -0.1 to 3.1
- x_block: float32 [16384, 64], P('row'), may hold values from -6 to 6
- r_block: float32 [16384, 64], P('row'), may hold values from -6 to 6
- p_block: float32 [16384, 64], P('row'), may hold values from -6 to 6
Outputs:
- x_next: float32 [16384, 64], P('row')
- r_next: float32 [16384, 64], P('row')
- p_next: float32 [16384, 64], P('row')
The draws below stay inside these ranges and needn't reach their ends.
All inputs are finite; a program needn't handle non-finite values.
Results may differ from the reference program's by a relative error of at most 0.0003.
Values sent between devices are 32-bit elements; how exact they have to be, the bound alone decides.
A program may use at most 192 MiB of HBM per device.

```python
import math
import jax
import jax.numpy as jnp
from jax import lax

N = 16384
K = 64
ITERS = 2
NS_STEPS = 8


def symmetric_field(key, spread, low, high):
    keys = jax.random.split(key, 2)
    noise = jax.random.normal(keys[0], (N, N), jnp.float32)
    mixed = (noise + noise.T) * (spread / math.sqrt(2.0 * N))
    diag_vals = jax.random.uniform(keys[1], (N,), jnp.float32, low, high)
    return mixed + jnp.diag(diag_vals)


def draw_a_matrix(key, part):
    return symmetric_field(jax.random.fold_in(key, 11), 0.5, -2.0, 2.0)


def draw_b_matrix(key, part):
    return symmetric_field(jax.random.fold_in(key, 23), 0.3, 1.5, 3.0)


def shard_levels(rng, shape, cuts, low, largest):
    level = 1.0
    for position, shards_of in cuts:
        heights = jax.random.uniform(jax.random.fold_in(jax.random.fold_in(rng, 6), position), (shards_of,), jnp.float32, low / len(cuts), largest / len(cuts))
        level = level * jnp.repeat(jnp.exp(heights), shape[position] // shards_of).reshape((-1,) + (1,) * (len(shape) - 1 - position))
    return level


def normal_values(own_key, shape, scale, most, cuts=(), held_as=jnp.bfloat16):
    entries = scale * jax.random.normal(own_key, shape, jnp.float32)
    if cuts:
        entries = entries * shard_levels(own_key, shape, cuts, -0.22, 0.18)
    return jnp.clip(entries, -most, most).astype(held_as)


def setup_inputs(seed: int = 0) -> dict:
    seeds = jax.random.split(jax.random.key(seed), 6)
    return {
        "a_matrix": draw_a_matrix(jax.random.fold_in(seeds[5], 71), 0),
        "b_matrix": draw_b_matrix(jax.random.fold_in(seeds[5], 71), 0),
        "x_block": normal_values(seeds[2], (N, K), 1.0, 6.0, ((0, 4),), jnp.float32),
        "r_block": normal_values(seeds[3], (N, K), 1.0, 6.0, ((0, 4),), jnp.float32),
        "p_block": normal_values(seeds[4], (N, K), 1.0, 6.0, ((0, 4),), jnp.float32),
    }


def matmul(left, right):
    return jnp.dot(left.astype(jnp.float32), right.astype(jnp.float32), precision=lax.Precision.HIGHEST, preferred_element_type=jnp.float32)

def ritz_step(gram_a, gram_b, count):
    gram_a = 0.5 * (gram_a + gram_a.T)
    gram_b = 0.5 * (gram_b + gram_b.T)
    lower = jnp.linalg.cholesky(gram_b)
    half = lax.linalg.triangular_solve(lower, gram_a, left_side=True, lower=True)
    middle = lax.linalg.triangular_solve(lower, half.T, left_side=True, lower=True)
    middle = 0.5 * (middle + middle.T)
    extent = middle.shape[0]
    ident = jnp.eye(extent, dtype=middle.dtype)
    shift = jnp.trace(middle) / extent
    centred = middle - shift * ident
    sign_est = centred / jnp.sqrt(jnp.sum(centred * centred) + 1e-06)
    for turn in range(NS_STEPS):
        sign_est = 1.5 * sign_est - 0.5 * matmul(sign_est, matmul(sign_est, sign_est))
    filtered = (0.5 * (ident - sign_est))[:, :count]
    coords = lax.linalg.triangular_solve(lower, filtered, left_side=True, lower=True, transpose_a=True) * math.sqrt(N)
    reduced = matmul(filtered.T, matmul(middle, filtered))
    return (coords, reduced)

def reference(a_matrix, b_matrix, x_block, r_block, p_block):
    for turn in range(ITERS):
        panel = jnp.concatenate([x_block, r_block, p_block], axis=1)
        prod_a = matmul(a_matrix, panel)
        prod_b = matmul(b_matrix, panel)
        coords, reduced = ritz_step(matmul(panel.T, prod_a), matmul(panel.T, prod_b), K)
        x_block = matmul(panel, coords)
        p_block = matmul(panel[:, K:], coords[K:])
        r_block = matmul(prod_a, coords) - matmul(matmul(prod_b, coords), reduced)
    return (x_block, r_block, p_block)
```

```python
import functools
import math

import jax
import jax.numpy as jnp
from jax import lax
from jax.experimental import pallas as pl
from jax.experimental.pallas import tpu as pltpu
from jax.sharding import PartitionSpec as P

NS_STEPS = 8
HIGHEST = lax.Precision.HIGHEST
HIGH = lax.Precision.HIGH


def mm(left, right, lc=1, rc=0, precision=HIGHEST):
    return lax.dot_general(
        left, right, (((lc,), (rc,)), ((), ())), precision=precision, preferred_element_type=jnp.float32
    )


MESH = pl.DeviceIdType.MESH


def remote(src, dst, send_sem, recv_sem, **where):
    return pltpu.make_async_remote_copy(
        src_ref=src, dst_ref=dst, send_sem=send_sem, recv_sem=recv_sem, device_id=where, device_id_type=MESH
    )


def greet(barrier, **where):
    pl.semaphore_signal(barrier, inc=1, device_id=where, device_id_type=MESH)


def meet(n_rows, others):
    r = lax.axis_index("row")
    barrier = pltpu.get_barrier_semaphore()
    has_up, has_down = r < n_rows - 1, r > 0

    @pl.when(has_up)
    def _():
        greet(barrier, row=r + 1)

    @pl.when(has_down)
    def _():
        greet(barrier, row=r - 1)

    @pl.when(has_up & has_down)
    def _():
        pl.semaphore_wait(barrier, others + 2)

    @pl.when(jnp.logical_not(has_up & has_down))
    def _():
        pl.semaphore_wait(barrier, others + 1)


def halves(value):
    high = value.astype(jnp.bfloat16)
    return high, (value - high.astype(jnp.float32)).astype(jnp.bfloat16)


def dot(left, right, lc=1, rc=0):
    return lax.dot_general(left, right, (((lc,), (rc,)), ((), ())), preferred_element_type=jnp.float32)


def apply_kernel(
    n_rows, n_cols, chunks, x_ref, a_ref, b_ref, on_a_ref, on_b_ref, tile_ref, x_parts, tile, up_sems, down_sems, recv_sems
):
    n, k = pl.program_id(0), pl.program_id(1)
    depth = pl.num_programs(1)
    now = n * depth + k
    steps = chunks
    m, tk = x_ref.shape[0], a_ref.shape[0]
    r, c = lax.axis_index("row"), lax.axis_index("col")
    ratio = n_cols // n_rows
    home, part = c // ratio, c % ratio
    width = tile.shape[1]
    step = width // chunks
    has_up, has_down = r < n_rows - 1, r > 0

    def slot(i):
        return tile.at[:, pl.ds(pl.multiple_of(i * step, 128), step)]

    def up(i, src):
        return remote(src, slot(i), up_sems.at[i], recv_sems.at[i], row=r + 1)

    def down(i, src):
        return remote(src, slot(i), down_sems.at[i], recv_sems.at[i], row=r - 1)

    def relay(i):
        @pl.when(r > home)
        def _():
            down(i, slot(i)).wait_recv()

            @pl.when(has_up)
            def _():
                up(i, slot(i)).start()

        @pl.when(r < home)
        def _():
            up(i, slot(i)).wait_recv()

            @pl.when(has_down)
            def _():
                down(i, slot(i)).start()

    @pl.when(now == 0)
    def _():
        meet(n_rows, 0)

        @pl.when(r == home)
        def _():
            for i in range(chunks):
                own = x_ref.at[:, pl.ds(pl.multiple_of(part * width + i * step, 128), step)]

                @pl.when(has_up)
                def _():
                    up(i, own).start()

                @pl.when(has_down)
                def _():
                    down(i, own).start()

        high, low = halves(x_ref[...])
        x_parts[:m] = high
        x_parts[m:] = low

    for mat_ref, out_ref in ((a_ref, on_a_ref), (b_ref, on_b_ref)):
        high, low = halves(mat_ref[...])
        x = x_parts[:, pl.ds(pl.multiple_of(k * tk, 128), tk)]
        both = dot(x, high)
        value = both[:m] + (both[m:] + dot(x[:m], low))

        @pl.when(k == 0)
        def _():
            out_ref[...] = value

        @pl.when(k > 0)
        def _():
            out_ref[...] += value

    for away in range(1, n_rows):
        lag = 2 * away

        @pl.when(((r == home + away) | (r == home - away)) & (now >= lag) & (now < chunks + lag))
        def _():
            relay(now - lag)

    @pl.when(now == steps - 1)
    def _():
        for away in range(1, n_rows):

            @pl.when((r == home + away) | (r == home - away))
            def _():
                for i in range(max(steps - 2 * away, 0), chunks):
                    relay(i)

        @pl.when((r >= home) & has_up)
        def _():
            for i in range(chunks):
                up(i, slot(i)).wait_send()

        @pl.when((r <= home) & has_down)
        def _():
            for i in range(chunks):
                down(i, slot(i)).wait_send()

        @pl.when(r == home)
        def _():
            tile_ref[...] = x_ref[:, pl.ds(pl.multiple_of(part * width, 128), width)]

        @pl.when(r != home)
        def _():
            tile_ref[...] = tile[...]


def apply_both(x_rows, a_matrix, b_matrix, collective_id):
    n_rows, n_cols = lax.axis_size("row"), lax.axis_size("col")
    m, rows = x_rows.shape
    cols = a_matrix.shape[1]
    tk, tn = min(1024, rows), min(512, cols)
    grid = (cols // tn, rows // tk)
    chunks = grid[0] * grid[1]
    block = pl.BlockSpec((tk, tn), lambda n, k: (k, n))
    out = pl.BlockSpec((m, tn), lambda n, k: (0, n))
    shape = jax.ShapeDtypeStruct((m, cols), jnp.float32)
    return pl.pallas_call(
        functools.partial(apply_kernel, n_rows, n_cols, chunks),
        out_shape=(shape,) * 3,
        grid=grid,
        in_specs=[pl.BlockSpec(memory_space=pltpu.VMEM), block, block],
        out_specs=[out, out, pl.BlockSpec(memory_space=pltpu.VMEM)],
        scratch_shapes=[pltpu.VMEM((2 * m, rows), jnp.bfloat16), pltpu.VMEM((m, cols), jnp.float32)]
        + [pltpu.SemaphoreType.DMA((chunks,))] * 3,
        compiler_params=pltpu.CompilerParams(
            collective_id=collective_id, has_side_effects=True, dimension_semantics=("arbitrary", "arbitrary")
        ),
        name="apply_both",
    )(x_rows, a_matrix, b_matrix)


LAG = 3


def gather_kernel(n_rows, n_cols, chunks, x_ref, o_ref, from_up, from_down, inward, row_send, up_recv, down_recv, send, recv):
    r, c = lax.axis_index("row"), lax.axis_index("col")
    ratio = n_cols // n_rows
    home, part = c // ratio, c % ratio
    width = x_ref.shape[1]
    step = width // chunks
    bits = n_cols.bit_length() - 1
    has_up, has_down = r < n_rows - 1, r > 0

    def bit(value, i):
        return value // 2**i % 2

    def flip(i):
        return c + 2**i * (1 - 2 * bit(c, i))

    barrier = pltpu.get_barrier_semaphore()
    for i in range(bits):
        greet(barrier, col=flip(i))
    meet(n_rows, bits)

    def lanes(ref, k):
        return ref.at[:, k * step : (k + 1) * step]

    def to_down(k, src):
        return remote(src, lanes(from_up, k), row_send.at[k], up_recv.at[k], row=r - 1)

    def to_up(k, src):
        return remote(src, lanes(from_down, k), row_send.at[k], down_recv.at[k], row=r + 1)

    def reduce(k):
        own = lanes(x_ref, k)

        @pl.when(r > home)
        def _():
            @pl.when(has_up)
            def _():
                to_down(k, own).wait_recv()
                lanes(inward, k)[...] = own[...] + lanes(from_up, k)[...]
                to_down(k, lanes(inward, k)).start()

            @pl.when(jnp.logical_not(has_up))
            def _():
                to_down(k, own).start()

        @pl.when(r < home)
        def _():
            @pl.when(has_down)
            def _():
                to_up(k, own).wait_recv()
                lanes(inward, k)[...] = own[...] + lanes(from_down, k)[...]
                to_up(k, lanes(inward, k)).start()

            @pl.when(jnp.logical_not(has_down))
            def _():
                to_up(k, own).start()

        @pl.when(r == home)
        def _():
            mine = o_ref.at[:, pl.ds(pl.multiple_of(part * width + k * step, 128), step)]

            @pl.when(has_up)
            def _():
                to_down(k, own).wait_recv()

            @pl.when(has_down)
            def _():
                to_up(k, own).wait_recv()

            @pl.when(has_up & has_down)
            def _():
                mine[...] = own[...] + (lanes(from_up, k)[...] + lanes(from_down, k)[...])

            @pl.when(jnp.logical_not(has_down))
            def _():
                mine[...] = own[...] + lanes(from_up, k)[...]

            @pl.when(jnp.logical_not(has_up))
            def _():
                mine[...] = own[...] + lanes(from_down, k)[...]

    def copies(p, k):
        apart = [(bit(c, i) + bit(r * ratio + p, i)) % 2 for i in range(bits)]
        top = [*range(bits - 1, 0, -1)]
        turn = k % len(top)
        order = [*top[turn:], *top[:turn], 0]
        spot = o_ref.at[:, p * width + k * step : p * width + (k + 1) * step]
        out = []
        for j, i in enumerate(order):
            later = sum(apart[x] for x in order[j:])
            out.append((later == 0, remote(spot, spot, send.at[p, k, j], recv.at[p, k], col=flip(i))))
        return out, sum(apart) > 0

    def broadcast(p, k, root):
        sends, inner = copies(p, k)

        @pl.when(jnp.logical_not(inner) if root else inner)
        def _():
            if not root:
                sends[0][1].wait_recv()
            for j, (condition, copy) in enumerate(sends):
                if root:
                    copy.start()
                elif j:

                    @pl.when(condition)
                    def _():
                        copy.start()

    for i in range(chunks + LAG):
        if i < chunks:
            reduce(i)
            for p in range(ratio):
                broadcast(p, i, True)
        if i >= LAG:
            for p in range(ratio):
                broadcast(p, i - LAG, False)
    for k in range(chunks):
        @pl.when(r > home)
        def _():
            to_down(k, lanes(x_ref, k)).wait_send()

        @pl.when(r < home)
        def _():
            to_up(k, lanes(x_ref, k)).wait_send()

        for p in range(ratio):
            for condition, copy in copies(p, k)[0]:

                @pl.when(condition)
                def _():
                    copy.wait_send()


def gather_sum(value, collective_id):
    n_rows, n_cols = lax.axis_size("row"), lax.axis_size("col")
    m, width = value.shape
    ratio = n_cols // n_rows
    chunks = min(8, width // 128)
    dma = pltpu.SemaphoreType.DMA
    return pl.pallas_call(
        functools.partial(gather_kernel, n_rows, n_cols, chunks),
        out_shape=jax.ShapeDtypeStruct((m, ratio * width), jnp.float32),
        in_specs=[pl.BlockSpec(memory_space=pltpu.VMEM)],
        out_specs=pl.BlockSpec(memory_space=pltpu.VMEM),
        scratch_shapes=[pltpu.VMEM((m, width), jnp.float32)] * 3
        + [dma((chunks,))] * 3
        + [dma((ratio, chunks, n_cols.bit_length() - 1)), dma((ratio, chunks))],
        compiler_params=pltpu.CompilerParams(collective_id=collective_id, has_side_effects=True),
        name="gather_sum",
    )(value)


def sum_kernel(n_rows, n_cols, over_rows, x_ref, o_ref, pair_buf, part, group_buf, row_buf, *sems):
    pair_send, pair_recv, group_send, group_recv, row_send, row_recv, all_send, all_recv, back_send, back_recv = sems
    r, c = lax.axis_index("row"), lax.axis_index("col")
    half = n_cols // 2
    g, h = c // 2, c % 2
    partner = 2 * g + 1 - h
    flat = len(x_ref.shape) == 2
    step = x_ref.shape[-1] // n_cols

    def piece(ref, index):
        return ref.at[:, pl.ds(pl.multiple_of(index * step, 128), step)] if flat else ref.at[index]

    barrier = pltpu.get_barrier_semaphore()
    greet(barrier, col=partner)
    for d in range(1, half):
        greet(barrier, col=2 * ((g + d) % half) + h)
    if over_rows:
        for e in range(1, n_rows):
            greet(barrier, row=(r + e) % n_rows)
    pl.semaphore_wait(barrier, half + (n_rows - 1 if over_rows else 0))

    order = [*range(1, half), 0]
    started = []
    pair = {}
    for d in order:
        j = (g + d) % half
        pair[d] = remote(piece(x_ref, (1 - h) * half + j), pair_buf.at[d], pair_send.at[d], pair_recv.at[d], col=partner)
        pair[d].start()
        started.append(pair[d])
    group = {}
    for d in order:
        j = (g + d) % half
        pair[d].wait_recv()
        value = piece(x_ref, h * half + j)[...] + pair_buf[d]
        if d:
            part[d] = value
            group[d] = remote(part.at[d], group_buf.at[d], group_send.at[d], group_recv.at[d], col=2 * j + h)
            group[d].start()
            started.append(group[d])
    for d in range(1, half):
        group[d].wait_recv()
        value = value + group_buf[d]
    if over_rows:
        row_buf[r] = value
        rows = []
        for e in range(1, n_rows):
            rows.append(remote(row_buf.at[r], row_buf.at[r], row_send.at[e], row_recv.at[e], row=(r + e) % n_rows))
            rows[-1].start()
        started.extend(rows)
        for e in range(1, n_rows):
            source = (r - e + n_rows) % n_rows
            remote(row_buf.at[source], row_buf.at[source], row_send.at[e], row_recv.at[e], row=source).wait_recv()
        value = row_buf[0]
        for e in range(1, n_rows):
            value = value + row_buf[e]
    mine = piece(o_ref, h * half + g)
    mine[...] = value
    for d in range(1, half):
        copy = remote(mine, mine, all_send.at[d], all_recv.at[d], col=2 * ((g + d) % half) + h)
        copy.start()
        started.append(copy)
    for d in range(half):
        j = (g - d + half) % half
        got = piece(o_ref, h * half + j)
        if d:
            remote(got, got, all_send.at[d], all_recv.at[d], col=2 * j + h).wait_recv()
        copy = remote(got, got, back_send.at[d], back_recv.at[d], col=partner)
        copy.start()
        started.append(copy)
    for d in range(half):
        got = piece(o_ref, (1 - h) * half + (g - d + half) % half)
        remote(got, got, back_send.at[d], back_recv.at[d], col=partner).wait_recv()
    for copy in started:
        copy.wait_send()


def sum_over(value, collective_id, over_rows):
    n_rows, n_cols = lax.axis_size("row"), lax.axis_size("col")
    half = n_cols // 2
    shape = (value.shape[0], value.shape[1] // n_cols) if value.ndim == 2 else value.shape[1:]
    dma = pltpu.SemaphoreType.DMA
    return pl.pallas_call(
        functools.partial(sum_kernel, n_rows, n_cols, over_rows),
        out_shape=jax.ShapeDtypeStruct(value.shape, jnp.float32),
        in_specs=[pl.BlockSpec(memory_space=pltpu.VMEM)],
        out_specs=pl.BlockSpec(memory_space=pltpu.VMEM),
        scratch_shapes=[pltpu.VMEM((half, *shape), jnp.float32)] * 3
        + [pltpu.VMEM((n_rows if over_rows else 1, *shape), jnp.float32)]
        + [dma((half,))] * 4
        + [dma((n_rows,))] * 2
        + [dma((half,))] * 4,
        compiler_params=pltpu.CompilerParams(collective_id=collective_id, has_side_effects=True),
        name="sum_over",
    )(value)


def total(value, collective_id):
    n_cols = lax.axis_size("col")
    rows, cols = value.shape
    return sum_over(value.reshape(n_cols, rows // n_cols, cols), collective_id, True).reshape(rows, cols)


def block_inverse(block):
    size = block.shape[0]
    rows = lax.broadcasted_iota(jnp.int32, (size, size), 0)
    cols = lax.broadcasted_iota(jnp.int32, (size, size), 1)
    inverse = jnp.where(rows == cols, 1.0, 0.0)
    for j in range(size):
        pivot = 1.0 / block[j : j + 1, j : j + 1]
        factor = jnp.where(rows[:, :1] > j, block[:, j : j + 1], 0.0)
        inverse = inverse - factor * (inverse[j : j + 1] * pivot)
        block = block - factor * (block[j : j + 1] * pivot)
    diag = jnp.sum(jnp.where(rows == cols, block, 0.0), axis=1, keepdims=True)
    return inverse / jnp.sqrt(diag)


def ritz_kernel(order, ga_ref, gb_ref, w_ref, ch_ref, wa_ref, wb_ref, linv_ref, sym_ref):
    n, k = w_ref.shape[0], ch_ref.shape[1]
    gb = gb_ref[...]
    sym_ref[...] = 0.5 * (gb + gb.T)
    ga = ga_ref[...]
    ga = 0.5 * (ga + ga.T)
    nb = n // k
    cut = lambda ref, i, j: ref[i * k : (i + 1) * k, j * k : (j + 1) * k]
    linv_ref[...] = jnp.zeros((n, n), jnp.float32)
    low, inv = {}, {}
    for j in range(nb):
        for i in range(j, nb):
            rest = cut(sym_ref, i, j)
            for m in range(j):
                rest = rest - mm(low[i, m], low[j, m], 1, 1)
            if i == j:
                inv[j, j] = block_inverse(rest)
            else:
                low[i, j] = mm(rest, inv[j, j], 1, 1)
    for j in range(nb):
        for i in range(j + 1, nb):
            total = mm(low[i, j], inv[j, j])
            for m in range(j + 1, i):
                total = total + mm(low[i, m], inv[m, j])
            inv[i, j] = -mm(inv[i, i], total)
    for (i, j), value in inv.items():
        linv_ref[i * k : (i + 1) * k, j * k : (j + 1) * k] = value
    linv = linv_ref[...]
    linv_t = linv.T
    middle = mm(mm(linv, ga), linv_t)
    middle = 0.5 * (middle + middle.T)
    rows = lax.broadcasted_iota(jnp.int32, (n, n), 0)
    cols = lax.broadcasted_iota(jnp.int32, (n, n), 1)
    ident = jnp.where(rows == cols, 1.0, 0.0)
    shift = jnp.sum(middle * ident) / n
    centred = middle - shift * ident
    sign_est = centred / jnp.sqrt(jnp.full((1, 1), jnp.sum(centred * centred) + 1e-06))
    for turn in range(NS_STEPS):
        sign_est = 1.5 * sign_est - 0.5 * mm(sign_est, mm(sign_est, sign_est))
    filtered = (0.5 * (ident - sign_est))[:, :k]
    coords = mm(linv_t, filtered) * math.sqrt(order)
    reduced = mm(filtered.T, mm(middle, filtered))
    ch_ref[...] = mm(coords, reduced)
    w_ref[:, :k] = coords
    w_ref[:, k:] = jnp.where(lax.broadcasted_iota(jnp.int32, (n, k), 0) >= k, coords, 0.0)
    w = w_ref[...]
    w_t = w.T
    wa_ref[...] = mm(w_t, mm(ga, w))
    wb_ref[...] = mm(w_t, mm(sym_ref[...], w))


def ritz(order, width, gram_a, gram_b):
    n, k = gram_a.shape[0], width
    shape = lambda *dims: jax.ShapeDtypeStruct(dims, jnp.float32)
    return pl.pallas_call(
        functools.partial(ritz_kernel, order),
        out_shape=(shape(n, 2 * k), shape(n, k), shape(2 * k, 2 * k), shape(2 * k, 2 * k)),
        in_specs=[pl.BlockSpec(memory_space=pltpu.VMEM)] * 2,
        out_specs=[pl.BlockSpec(memory_space=pltpu.VMEM)] * 4,
        scratch_shapes=[pltpu.VMEM((n, n), jnp.float32)] * 2,
        name="ritz",
    )(gram_a, gram_b)


def extend(kept, fresh):
    k = fresh.shape[1]
    x, r, p = fresh[:k], fresh[k : 2 * k], fresh[2 * k :]
    return jnp.concatenate(
        [
            jnp.concatenate([kept[:k, :k], x, kept[:k, k:]], axis=1),
            jnp.concatenate([x.T, r, p.T], axis=1),
            jnp.concatenate([kept[k:, :k], p, kept[k:, k:]], axis=1),
        ],
        axis=0,
    )


def local(order, a_matrix, b_matrix, x_block, r_block, p_block):
    k = x_block.shape[1]
    panel = jnp.concatenate([x_block.T, r_block.T, p_block.T], axis=0)
    prod_a, prod_b, tile = apply_both(panel, a_matrix, b_matrix, 0)
    grams = total(jnp.concatenate([mm(tile, prod_a, 1, 1), mm(tile, prod_b, 1, 1)], axis=1), 1)
    w, ch, kept_a, kept_b = ritz(order, k, grams[:, : 3 * k], grams[:, 3 * k :])
    coords = w[:, :k]
    resid = gather_sum(mm(coords, prod_a, 0, 0) - mm(ch, prod_b, 0, 0), 2)
    fresh_a, fresh_b, resid_tile = apply_both(resid, a_matrix, b_matrix, 3)
    both = mm(w, tile, 0, 0)
    tile = jnp.concatenate([both[:k], resid_tile, both[k:]], axis=0)
    grams = total(jnp.concatenate([mm(tile, fresh_a, 1, 1), mm(tile, fresh_b, 1, 1)], axis=1), 4)
    w2, ch2, _, _ = ritz(order, k, extend(kept_a, grams[:, :k]), extend(kept_b, grams[:, k:]))
    c2 = w2[:, :k]
    outer = lambda c: jnp.concatenate([c[:k], c[2 * k :]], axis=0)
    on_a, on_b = mm(w, outer(c2)), mm(w, outer(ch2))
    last = gather_sum(
        (mm(on_a, prod_a, 0, 0) + mm(c2[k : 2 * k], fresh_a, 0, 0))
        - (mm(on_b, prod_b, 0, 0) + mm(ch2[k : 2 * k], fresh_b, 0, 0)),
        5,
    )
    both = mm(w, panel, 0, 0)
    panel = jnp.concatenate([both[:k], resid, both[k:]], axis=0)
    both = mm(w2, panel, 0, 0)
    return (both[:k].T, last.T, both[k:].T)


def solution(mesh):
    def whole(a_matrix, b_matrix, x_block, r_block, p_block):
        return jax.shard_map(
            functools.partial(local, a_matrix.shape[0]),
            mesh=mesh,
            in_specs=(P("row", "col"), P("row", "col"), P("row", None), P("row", None), P("row", None)),
            out_specs=(P("row", None), P("row", None), P("row", None)),
            check_vma=False,
        )(a_matrix, b_matrix, x_block, r_block, p_block)

    return whole
```

```python
import functools
import math

import jax
import jax.numpy as jnp
from jax import lax
from jax.experimental import pallas as pl
from jax.experimental.pallas import tpu as pltpu
from jax.sharding import PartitionSpec as P

NS_STEPS = 8
HIGHEST = lax.Precision.HIGHEST
HIGH = lax.Precision.HIGH


def mm(left, right, lc=1, rc=0, precision=HIGHEST):
    return lax.dot_general(
        left, right, (((lc,), (rc,)), ((), ())), precision=precision, preferred_element_type=jnp.float32
    )


MESH = pl.DeviceIdType.MESH


def remote(src, dst, send_sem, recv_sem, **where):
    return pltpu.make_async_remote_copy(
        src_ref=src, dst_ref=dst, send_sem=send_sem, recv_sem=recv_sem, device_id=where, device_id_type=MESH
    )


def greet(barrier, **where):
    pl.semaphore_signal(barrier, inc=1, device_id=where, device_id_type=MESH)


def meet(n_rows, others):
    r = lax.axis_index("row")
    barrier = pltpu.get_barrier_semaphore()
    has_up, has_down = r < n_rows - 1, r > 0

    @pl.when(has_up)
    def _():
        greet(barrier, row=r + 1)

    @pl.when(has_down)
    def _():
        greet(barrier, row=r - 1)

    @pl.when(has_up & has_down)
    def _():
        pl.semaphore_wait(barrier, others + 2)

    @pl.when(jnp.logical_not(has_up & has_down))
    def _():
        pl.semaphore_wait(barrier, others + 1)


def halves(value):
    high = value.astype(jnp.bfloat16)
    return high, (value - high.astype(jnp.float32)).astype(jnp.bfloat16)


def dot(left, right, lc=1, rc=0):
    return lax.dot_general(left, right, (((lc,), (rc,)), ((), ())), preferred_element_type=jnp.float32)


def apply_kernel(
    n_rows, n_cols, chunks, steps, x_ref, a_ref, b_ref, out_ref, tile_ref, x_parts, tile, up_sems, down_sems, recv_sems
):
    n, k = pl.program_id(0), pl.program_id(1)
    depth = pl.num_programs(1)
    now = n * depth + k
    per = chunks // steps
    m, tk = x_ref.shape[0], a_ref.shape[0]
    r, c = lax.axis_index("row"), lax.axis_index("col")
    ratio = n_cols // n_rows
    home, part = c // ratio, c % ratio
    width = tile.shape[1]
    step = width // chunks
    has_up, has_down = r < n_rows - 1, r > 0

    def slot(i):
        return tile.at[:, pl.ds(pl.multiple_of(i * step, 128), step)]

    def up(i, src):
        return remote(src, slot(i), up_sems.at[i], recv_sems.at[i], row=r + 1)

    def down(i, src):
        return remote(src, slot(i), down_sems.at[i], recv_sems.at[i], row=r - 1)

    def relay(i):
        @pl.when(r > home)
        def _():
            down(i, slot(i)).wait_recv()

            @pl.when(has_up)
            def _():
                up(i, slot(i)).start()

        @pl.when(r < home)
        def _():
            up(i, slot(i)).wait_recv()

            @pl.when(has_down)
            def _():
                down(i, slot(i)).start()

    @pl.when(now == 0)
    def _():
        meet(n_rows, 0)

        @pl.when(r == home)
        def _():
            for i in range(chunks):
                own = x_ref.at[:, pl.ds(pl.multiple_of(part * width + i * step, 128), step)]

                @pl.when(has_up)
                def _():
                    up(i, own).start()

                @pl.when(has_down)
                def _():
                    down(i, own).start()

        high, low = halves(x_ref[...])
        x_parts[:m] = high
        x_parts[m:] = low

    for at, mat_ref in enumerate((a_ref, b_ref)):
        high, low = halves(mat_ref[...])
        x = x_parts[:, pl.ds(pl.multiple_of(k * tk, 128), tk)]
        both = dot(x, high)
        value = both[:m] + (both[m:] + dot(x[:m], low))

        @pl.when(k == 0)
        def _():
            out_ref[at * m : (at + 1) * m] = value

        @pl.when(k > 0)
        def _():
            out_ref[at * m : (at + 1) * m] += value

    for away in range(1, n_rows):
        for i in range(per):
            chunk = per * now + i - 2 * away

            @pl.when(((r == home + away) | (r == home - away)) & (chunk >= 0) & (chunk < chunks))
            def _():
                relay(chunk)

    @pl.when(now == steps - 1)
    def _():
        for away in range(1, n_rows):

            @pl.when((r == home + away) | (r == home - away))
            def _():
                for i in range(max(chunks - 2 * away, 0), chunks):
                    relay(i)

        @pl.when((r >= home) & has_up)
        def _():
            for i in range(chunks):
                up(i, slot(i)).wait_send()

        @pl.when((r <= home) & has_down)
        def _():
            for i in range(chunks):
                down(i, slot(i)).wait_send()

        @pl.when(r == home)
        def _():
            tile_ref[...] = x_ref[:, pl.ds(pl.multiple_of(part * width, 128), width)]

        @pl.when(r != home)
        def _():
            tile_ref[...] = tile[...]


TK, TN = 4096, 256


def apply_both(x_rows, a_matrix, b_matrix, collective_id):
    n_rows, n_cols = lax.axis_size("row"), lax.axis_size("col")
    m, rows = x_rows.shape
    cols = a_matrix.shape[1]
    tk, tn = min(TK, rows), min(TN, cols)
    grid = (cols // tn, rows // tk)
    steps = grid[0] * grid[1]
    chunks = max(steps, cols // 128)
    block = pl.BlockSpec((tk, tn), lambda n, k: (k, n))
    shape = lambda rows: jax.ShapeDtypeStruct((rows, cols), jnp.float32)
    return pl.pallas_call(
        functools.partial(apply_kernel, n_rows, n_cols, chunks, steps),
        out_shape=(shape(2 * m), shape(m)),
        grid=grid,
        in_specs=[pl.BlockSpec(memory_space=pltpu.VMEM), block, block],
        out_specs=[pl.BlockSpec((2 * m, tn), lambda n, k: (0, n)), pl.BlockSpec(memory_space=pltpu.VMEM)],
        scratch_shapes=[pltpu.VMEM((2 * m, rows), jnp.bfloat16), pltpu.VMEM((m, cols), jnp.float32)]
        + [pltpu.SemaphoreType.DMA((chunks,))] * 3,
        compiler_params=pltpu.CompilerParams(
            collective_id=collective_id, has_side_effects=True, dimension_semantics=("arbitrary", "arbitrary")
        ),
        name="apply_both",
    )(x_rows, a_matrix, b_matrix)


def gather_kernel(n_rows, n_cols, chunks, x_ref, o_ref, from_up, from_down, inward, row_send, up_recv, down_recv, send, recv):
    r, c = lax.axis_index("row"), lax.axis_index("col")
    ratio = n_cols // n_rows
    home, part = c // ratio, c % ratio
    width = x_ref.shape[1]
    step = width // chunks
    bits = n_cols.bit_length() - 1
    has_up, has_down = r < n_rows - 1, r > 0

    def bit(value, i):
        return value // 2**i % 2

    def flip(i):
        return c + 2**i * (1 - 2 * bit(c, i))

    barrier = pltpu.get_barrier_semaphore()
    for i in range(bits):
        greet(barrier, col=flip(i))
    meet(n_rows, bits)

    def lanes(ref, k):
        return ref.at[:, k * step : (k + 1) * step]

    def to_down(k, src):
        return remote(src, lanes(from_up, k), row_send.at[k], up_recv.at[k], row=r - 1)

    def to_up(k, src):
        return remote(src, lanes(from_down, k), row_send.at[k], down_recv.at[k], row=r + 1)

    def reduce(k):
        own = lanes(x_ref, k)

        @pl.when(r > home)
        def _():
            @pl.when(has_up)
            def _():
                to_down(k, own).wait_recv()
                lanes(inward, k)[...] = own[...] + lanes(from_up, k)[...]
                to_down(k, lanes(inward, k)).start()

            @pl.when(jnp.logical_not(has_up))
            def _():
                to_down(k, own).start()

        @pl.when(r < home)
        def _():
            @pl.when(has_down)
            def _():
                to_up(k, own).wait_recv()
                lanes(inward, k)[...] = own[...] + lanes(from_down, k)[...]
                to_up(k, lanes(inward, k)).start()

            @pl.when(jnp.logical_not(has_down))
            def _():
                to_up(k, own).start()

        @pl.when(r == home)
        def _():
            mine = o_ref.at[:, pl.ds(pl.multiple_of(part * width + k * step, 128), step)]

            @pl.when(has_up)
            def _():
                to_down(k, own).wait_recv()

            @pl.when(has_down)
            def _():
                to_up(k, own).wait_recv()

            @pl.when(has_up & has_down)
            def _():
                mine[...] = own[...] + (lanes(from_up, k)[...] + lanes(from_down, k)[...])

            @pl.when(jnp.logical_not(has_down))
            def _():
                mine[...] = own[...] + lanes(from_up, k)[...]

            @pl.when(jnp.logical_not(has_up))
            def _():
                mine[...] = own[...] + lanes(from_down, k)[...]

    def copies(p, k):
        apart = [(bit(c, i) + bit(r * ratio + p, i)) % 2 for i in range(bits)]
        top = [*range(bits - 1, 0, -1)]
        turn = k % len(top)
        order = [*top[turn:], *top[:turn], 0]
        spot = o_ref.at[:, p * width + k * step : p * width + (k + 1) * step]
        out = []
        for j, i in enumerate(order):
            later = sum(apart[x] for x in order[j:])
            out.append((later == 0, remote(spot, spot, send.at[p, k, j], recv.at[p, k], col=flip(i))))
        return out, sum(apart) > 0

    def broadcast(p, k, root):
        sends, inner = copies(p, k)

        @pl.when(jnp.logical_not(inner) if root else inner)
        def _():
            if not root:
                sends[0][1].wait_recv()
            for j, (condition, copy) in enumerate(sends):
                if root:
                    copy.start()
                elif j:

                    @pl.when(condition)
                    def _():
                        copy.start()

    for i in range(chunks):
        reduce(i)
        for p in range(ratio):
            broadcast(p, i, True)
    for i in range(chunks):
        for p in range(ratio):
            broadcast(p, i, False)
    for k in range(chunks):
        @pl.when(r > home)
        def _():
            to_down(k, lanes(x_ref, k)).wait_send()

        @pl.when(r < home)
        def _():
            to_up(k, lanes(x_ref, k)).wait_send()

        for p in range(ratio):
            for condition, copy in copies(p, k)[0]:

                @pl.when(condition)
                def _():
                    copy.wait_send()


def gather_sum(value, collective_id):
    n_rows, n_cols = lax.axis_size("row"), lax.axis_size("col")
    m, width = value.shape
    ratio = n_cols // n_rows
    chunks = min(8, width // 128)
    dma = pltpu.SemaphoreType.DMA
    return pl.pallas_call(
        functools.partial(gather_kernel, n_rows, n_cols, chunks),
        out_shape=jax.ShapeDtypeStruct((m, ratio * width), jnp.float32),
        in_specs=[pl.BlockSpec(memory_space=pltpu.VMEM)],
        out_specs=pl.BlockSpec(memory_space=pltpu.VMEM),
        scratch_shapes=[pltpu.VMEM((m, width), jnp.float32)] * 3
        + [dma((chunks,))] * 3
        + [dma((ratio, chunks, n_cols.bit_length() - 1)), dma((ratio, chunks))],
        compiler_params=pltpu.CompilerParams(collective_id=collective_id, has_side_effects=True),
        name="gather_sum",
    )(value)


def sum_kernel(n_rows, n_cols, over_rows, x_ref, o_ref, pair_buf, part, group_buf, row_buf, *sems):
    pair_send, pair_recv, group_send, group_recv, row_send, row_recv, all_send, all_recv, back_send, back_recv = sems
    r, c = lax.axis_index("row"), lax.axis_index("col")
    half = n_cols // 2
    g, h = c // 2, c % 2
    partner = 2 * g + 1 - h
    flat = len(x_ref.shape) == 2
    step = x_ref.shape[-1] // n_cols

    def piece(ref, index):
        return ref.at[:, pl.ds(pl.multiple_of(index * step, 128), step)] if flat else ref.at[index]

    barrier = pltpu.get_barrier_semaphore()
    greet(barrier, col=partner)
    for d in range(1, half):
        greet(barrier, col=2 * ((g + d) % half) + h)
    if over_rows:
        for e in range(1, n_rows):
            greet(barrier, row=(r + e) % n_rows)
    pl.semaphore_wait(barrier, half + (n_rows - 1 if over_rows else 0))

    order = [*range(1, half), 0]
    started = []
    pair = {}
    for d in order:
        j = (g + d) % half
        pair[d] = remote(piece(x_ref, (1 - h) * half + j), pair_buf.at[d], pair_send.at[d], pair_recv.at[d], col=partner)
        pair[d].start()
        started.append(pair[d])
    group = {}
    for d in order:
        j = (g + d) % half
        pair[d].wait_recv()
        value = piece(x_ref, h * half + j)[...] + pair_buf[d]
        if d:
            part[d] = value
            group[d] = remote(part.at[d], group_buf.at[d], group_send.at[d], group_recv.at[d], col=2 * j + h)
            group[d].start()
            started.append(group[d])
    for d in range(1, half):
        group[d].wait_recv()
        value = value + group_buf[d]
    if over_rows:
        row_buf[r] = value
        rows = []
        for e in range(1, n_rows):
            rows.append(remote(row_buf.at[r], row_buf.at[r], row_send.at[e], row_recv.at[e], row=(r + e) % n_rows))
            rows[-1].start()
        started.extend(rows)
        for e in range(1, n_rows):
            source = (r - e + n_rows) % n_rows
            remote(row_buf.at[source], row_buf.at[source], row_send.at[e], row_recv.at[e], row=source).wait_recv()
        value = row_buf[0]
        for e in range(1, n_rows):
            value = value + row_buf[e]
    mine = piece(o_ref, h * half + g)
    mine[...] = value
    for d in range(1, half):
        copy = remote(mine, mine, all_send.at[d], all_recv.at[d], col=2 * ((g + d) % half) + h)
        copy.start()
        started.append(copy)
    for d in range(half):
        j = (g - d + half) % half
        got = piece(o_ref, h * half + j)
        if d:
            remote(got, got, all_send.at[d], all_recv.at[d], col=2 * j + h).wait_recv()
        copy = remote(got, got, back_send.at[d], back_recv.at[d], col=partner)
        copy.start()
        started.append(copy)
    for d in range(half):
        got = piece(o_ref, (1 - h) * half + (g - d + half) % half)
        remote(got, got, back_send.at[d], back_recv.at[d], col=partner).wait_recv()
    for copy in started:
        copy.wait_send()


def sum_over(value, collective_id, over_rows):
    n_rows, n_cols = lax.axis_size("row"), lax.axis_size("col")
    half = n_cols // 2
    shape = (value.shape[0], value.shape[1] // n_cols) if value.ndim == 2 else value.shape[1:]
    dma = pltpu.SemaphoreType.DMA
    return pl.pallas_call(
        functools.partial(sum_kernel, n_rows, n_cols, over_rows),
        out_shape=jax.ShapeDtypeStruct(value.shape, jnp.float32),
        in_specs=[pl.BlockSpec(memory_space=pltpu.VMEM)],
        out_specs=pl.BlockSpec(memory_space=pltpu.VMEM),
        scratch_shapes=[pltpu.VMEM((half, *shape), jnp.float32)] * 3
        + [pltpu.VMEM((n_rows if over_rows else 1, *shape), jnp.float32)]
        + [dma((half,))] * 4
        + [dma((n_rows,))] * 2
        + [dma((half,))] * 4,
        compiler_params=pltpu.CompilerParams(collective_id=collective_id, has_side_effects=True),
        name="sum_over",
    )(value)


def total(value, collective_id):
    n_cols = lax.axis_size("col")
    rows, cols = value.shape
    return sum_over(value.reshape(n_cols, rows // n_cols, cols), collective_id, True)


PANEL = 8


def block_inverse(block):
    size = block.shape[0]
    shape = (size, 2 * size)
    rows = lax.broadcasted_iota(jnp.int32, shape, 0)
    cols = lax.broadcasted_iota(jnp.int32, shape, 1)
    ident = jnp.where(rows == cols, 1.0, 0.0)[:, :size]
    work = jnp.concatenate([block, ident], axis=1)
    for start in range(0, size, PANEL):
        spread = [jnp.broadcast_to(work[:, start + i : start + i + 1], shape) for i in range(PANEL)]
        for i in range(PANEL):
            j = start + i
            column = spread[i]
            factor = jnp.where(rows > j, column, 0.0) * (1.0 / column[j : j + 1])
            for later in range(i + 1, PANEL):
                spread[later] = spread[later] - factor * column[start + later : start + later + 1]
            work = work - factor * work[j : j + 1]
    diag = jnp.sum(jnp.where(rows == cols, work, 0.0), axis=1, keepdims=True)
    return work[:, size:] / jnp.sqrt(diag)


def mm_split(left, right):
    left_high, left_low = halves(left)
    right_high, right_low = halves(right)
    return dot(left_high, right_high) + (dot(left_high, right_low) + dot(left_low, right_high))


def solve(order, k, ga, gb, linv_ref, sym_ref):
    n = ga.shape[0]
    sym_ref[...] = gb
    nb = n // k
    cut = lambda ref, i, j: ref[i * k : (i + 1) * k, j * k : (j + 1) * k]
    linv_ref[...] = jnp.zeros((n, n), jnp.float32)
    low, inv = {}, {}
    for j in range(nb):
        for i in range(j, nb):
            rest = cut(sym_ref, i, j)
            for m in range(j):
                rest = rest - mm(low[i, m], low[j, m], 1, 1)
            if i == j:
                inv[j, j] = block_inverse(rest)
            else:
                low[i, j] = mm(rest, inv[j, j], 1, 1)
    for j in range(nb):
        for i in range(j + 1, nb):
            total = mm(low[i, j], inv[j, j])
            for m in range(j + 1, i):
                total = total + mm(low[i, m], inv[m, j])
            inv[i, j] = -mm(inv[i, i], total)
    for (i, j), value in inv.items():
        linv_ref[i * k : (i + 1) * k, j * k : (j + 1) * k] = value
    linv = linv_ref[...]
    linv_t = linv.T
    middle = mm(mm(linv, ga), linv_t)
    middle = 0.5 * (middle + middle.T)
    rows = lax.broadcasted_iota(jnp.int32, (n, n), 0)
    cols = lax.broadcasted_iota(jnp.int32, (n, n), 1)
    ident = jnp.where(rows == cols, 1.0, 0.0)
    shift = jnp.sum(middle * ident) / n
    centred = middle - shift * ident
    sign_est = centred / jnp.sqrt(jnp.full((1, 1), jnp.sum(centred * centred) + 1e-06))
    for turn in range(NS_STEPS):
        sign_est = 1.5 * sign_est - 0.5 * mm_split(sign_est, mm_split(sign_est, sign_est))
    filtered = (0.5 * (ident - sign_est))[:, :k]
    coords = mm(linv_t, filtered) * math.sqrt(order)
    reduced = mm(filtered.T, mm(middle, filtered))
    return coords, mm(coords, reduced)


def outer_rows(value, k):
    return jnp.where((lax.broadcasted_iota(jnp.int32, value.shape, 0) >= k), value, 0.0)


def first_kernel(order, grams_ref, w_ref, mix_ref, wa_ref, wb_ref, linv_ref, sym_ref):
    n, k = w_ref.shape[0], mix_ref.shape[1]
    grams = grams_ref[...].reshape(2 * n, n)
    ga, gb = grams[:n], grams[n:]
    ga, gb = 0.5 * (ga + ga.T), 0.5 * (gb + gb.T)
    coords, reduced = solve(order, k, ga, gb, linv_ref, sym_ref)
    mix_ref[:n] = coords
    mix_ref[n:] = -reduced
    w_ref[:, :k] = coords
    w_ref[:, k:] = outer_rows(coords, k)
    w = w_ref[...]
    w_t = w.T
    wa_ref[...] = mm(w_t, mm(ga, w))
    wb_ref[...] = mm(w_t, mm(sym_ref[...], w))


def second_kernel(order, wa_ref, wb_ref, w_ref, grams_ref, wide_ref, inner_ref, mix_ref, mix_in_ref, linv_ref, sym_ref, ga_ref, c_ref):
    n, k = w_ref.shape[0], mix_ref.shape[1]
    grams = grams_ref[...].reshape(2 * k, n + k)
    w = w_ref[...]
    for at, kept in enumerate((wa_ref, wb_ref)):
        fresh = grams[at * k : (at + 1) * k]
        ends = mm(fresh[:, :n], w)
        middle = fresh[:, n:]
        full = ga_ref.at[at]
        full[:k, :k] = kept[:k, :k]
        full[:k, 2 * k :] = kept[:k, k:]
        full[2 * k :, :k] = kept[k:, :k]
        full[2 * k :, 2 * k :] = kept[k:, k:]
        full[k : 2 * k, :k] = ends[:, :k]
        full[k : 2 * k, 2 * k :] = ends[:, k:]
        full[k : 2 * k, k : 2 * k] = middle
        full[:k, k : 2 * k] = ends[:, :k].T
        full[2 * k :, k : 2 * k] = ends[:, k:].T
    ga, gb = ga_ref[0], ga_ref[1]
    ga, gb = 0.5 * (ga + ga.T), 0.5 * (gb + gb.T)
    coords, reduced = solve(order, k, ga, gb, linv_ref, sym_ref)
    c_ref[:, :k] = coords
    c_ref[:, k : 2 * k] = outer_rows(coords, k)
    c_ref[:, 2 * k :] = reduced
    ends = mm(w[:, :k], c_ref[:k]) + mm(w[:, k:], c_ref[2 * k :])
    wide_ref[...] = ends[:, : 2 * k]
    inner_ref[...] = c_ref[k : 2 * k, : 2 * k]
    mix_ref[:n] = ends[:, :k]
    mix_ref[n:] = -ends[:, 2 * k :]
    mix_in_ref[:k] = c_ref[k : 2 * k, :k]
    mix_in_ref[k:] = -c_ref[k : 2 * k, 2 * k :]


def in_vmem(kernel, shapes, scratch, name, *args):
    return pl.pallas_call(
        kernel,
        out_shape=tuple(jax.ShapeDtypeStruct(dims, jnp.float32) for dims in shapes),
        in_specs=[pl.BlockSpec(memory_space=pltpu.VMEM)] * len(args),
        out_specs=[pl.BlockSpec(memory_space=pltpu.VMEM)] * len(shapes),
        scratch_shapes=[pltpu.VMEM(dims, jnp.float32) for dims in scratch],
        name=name,
    )(*args)


def first_ritz(order, k, grams):
    n = grams.shape[-1]
    shapes = ((n, 2 * k), (2 * n, k), (2 * k, 2 * k), (2 * k, 2 * k))
    return in_vmem(functools.partial(first_kernel, order), shapes, [(n, n)] * 2, "first_ritz", grams)


def second_ritz(order, k, kept_a, kept_b, w, grams):
    n = w.shape[0]
    shapes = ((n, 2 * k), (k, 2 * k), (2 * n, k), (2 * k, k))
    scratch = [(n, n)] * 2 + [(2, n, n), (n, 3 * k)]
    return in_vmem(functools.partial(second_kernel, order), shapes, scratch, "second_ritz", kept_a, kept_b, w, grams)


def local(order, a_matrix, b_matrix, x_block, r_block, p_block):
    k = x_block.shape[1]
    panel = jnp.concatenate([x_block.T, r_block.T, p_block.T], axis=0)
    prods, tile = apply_both(panel, a_matrix, b_matrix, 0)
    grams = total(mm(prods, tile, 1, 1, HIGH), 1)
    w, mix, kept_a, kept_b = first_ritz(order, k, grams)
    resid = gather_sum(mm(mix, prods, 0, 0, HIGH), 2)
    fresh, resid_tile = apply_both(resid, a_matrix, b_matrix, 3)
    grams = total(mm(fresh, jnp.concatenate([tile, resid_tile], axis=0), 1, 1, HIGH), 4)
    wide, inner, mix, mix_in = second_ritz(order, k, kept_a, kept_b, w, grams)
    last = gather_sum(mm(mix, prods, 0, 0, HIGH) + mm(mix_in, fresh, 0, 0, HIGH), 5)
    both = mm(wide, panel, 0, 0, HIGH) + mm(inner, resid, 0, 0, HIGH)
    return (both[:k].T, last.T, both[k:].T)


def solution(mesh):
    def whole(a_matrix, b_matrix, x_block, r_block, p_block):
        return jax.shard_map(
            functools.partial(local, a_matrix.shape[0]),
            mesh=mesh,
            in_specs=(P("row", "col"), P("row", "col"), P("row", None), P("row", None), P("row", None)),
            out_specs=(P("row", None), P("row", None), P("row", None)),
            check_vma=False,
        )(a_matrix, b_matrix, x_block, r_block, p_block)

    return whole
```

```python
import functools
import itertools
import math

import jax
import jax.numpy as jnp
from jax import lax
from jax.experimental import pallas as pl
from jax.experimental.pallas import tpu as pltpu
from jax.sharding import PartitionSpec as P

NS_STEPS = 8
HIGHEST = lax.Precision.HIGHEST
HIGH = lax.Precision.HIGH


def mm(left, right, lc=1, rc=0, precision=HIGHEST):
    return lax.dot_general(
        left, right, (((lc,), (rc,)), ((), ())), precision=precision, preferred_element_type=jnp.float32
    )


MESH = pl.DeviceIdType.MESH


def remote(src, dst, send_sem, recv_sem, **where):
    return pltpu.make_async_remote_copy(
        src_ref=src, dst_ref=dst, send_sem=send_sem, recv_sem=recv_sem, device_id=where, device_id_type=MESH
    )


def greet(barrier, **where):
    pl.semaphore_signal(barrier, inc=1, device_id=where, device_id_type=MESH)


def meet(n_rows, others):
    r = lax.axis_index("row")
    barrier = pltpu.get_barrier_semaphore()
    has_up, has_down = r < n_rows - 1, r > 0

    @pl.when(has_up)
    def _():
        greet(barrier, row=r + 1)

    @pl.when(has_down)
    def _():
        greet(barrier, row=r - 1)

    @pl.when(has_up & has_down)
    def _():
        pl.semaphore_wait(barrier, others + 2)

    @pl.when(jnp.logical_not(has_up & has_down))
    def _():
        pl.semaphore_wait(barrier, others + 1)


def halves(value):
    high = value.astype(jnp.bfloat16)
    return high, (value - high.astype(jnp.float32)).astype(jnp.bfloat16)


def dot(left, right, lc=1, rc=0):
    return lax.dot_general(left, right, (((lc,), (rc,)), ((), ())), preferred_element_type=jnp.float32)


def mirror_pairs(n):
    pairs = list(itertools.combinations(range(n), 2))
    if len(pairs) > 6:
        return [(low, high) for low, high in pairs]
    best = None
    for flips in itertools.product((False, True), repeat=len(pairs)):
        chosen = [(high, low) if flip else (low, high) for flip, (low, high) in zip(flips, pairs)]
        loads = {}
        for row, home in chosen:
            for z in range(min(row, home), max(row, home)):
                link = (home, row > home, z)
                loads[link] = loads.get(link, 0) + 1
        if best is None or max(loads.values()) < best[0]:
            best = (max(loads.values()), chosen)
    return best[1]


def apply_kernel(n_rows, n_cols, steps, x_ref, a_ref, b_ref, out_ref, tile_ref, x_parts, tile, send_sems, recv_sem):
    n, k = pl.program_id(0), pl.program_id(1)
    now = n * pl.num_programs(1) + k
    m, tk = x_ref.shape[0], a_ref.shape[0]
    r, c = lax.axis_index("row"), lax.axis_index("col")
    ratio = n_cols // n_rows
    home, part = c // ratio, c % ratio
    width = tile.shape[1]
    pairs = mirror_pairs(n_rows)
    targets = {q: [row for row, at in pairs if at == q] for q in range(n_rows)}
    own = x_ref.at[:, pl.ds(pl.multiple_of(part * width, 128), width)]

    def send(i, row):
        return remote(own, tile, send_sems.at[i], recv_sem.at[0], row=row)

    @pl.when(now == 0)
    def _():
        barrier = pltpu.get_barrier_semaphore()
        for q in range(n_rows):

            @pl.when((r == q) & (home == q))
            def _():
                for row in targets[q]:
                    greet(barrier, row=row)
                if targets[q]:
                    pl.semaphore_wait(barrier, len(targets[q]))
                for i, row in enumerate(targets[q]):
                    send(i, row).start()

            for row in targets[q]:

                @pl.when((r == row) & (home == q))
                def _():
                    greet(barrier, row=q)
                    pl.semaphore_wait(barrier, 1)

        high, low = halves(x_ref[...])
        x_parts[:m] = high
        x_parts[m:] = low

    for at, mat_ref in enumerate((a_ref, b_ref)):
        high, low = halves(mat_ref[...])
        x = x_parts[:, pl.ds(pl.multiple_of(k * tk, 128), tk)]
        both = dot(x, high)
        value = both[:m] + (both[m:] + dot(x[:m], low))

        @pl.when(k == 0)
        def _():
            out_ref[at * m : (at + 1) * m] = value

        @pl.when(k > 0)
        def _():
            out_ref[at * m : (at + 1) * m] += value

    @pl.when(now == steps - 1)
    def _():
        for q in range(n_rows):

            @pl.when((r == q) & (home == q))
            def _():
                for i, row in enumerate(targets[q]):
                    send(i, row).wait_send()
                tile_ref[...] = own[...]

            for row in range(n_rows):
                if row in targets[q]:

                    @pl.when((r == row) & (home == q))
                    def _():
                        send(0, q).wait_recv()
                        tile_ref[...] = 2.0 * tile[...]

                elif row != q:

                    @pl.when((r == row) & (home == q))
                    def _():
                        tile_ref[...] = jnp.zeros_like(tile_ref)


TK, TN = 4096, 256


def apply_both(x_rows, a_matrix, b_matrix, collective_id):
    n_rows, n_cols = lax.axis_size("row"), lax.axis_size("col")
    m, rows = x_rows.shape
    cols = a_matrix.shape[1]
    tk, tn = min(TK, rows), min(TN, cols)
    grid = (cols // tn, rows // tk)
    block = pl.BlockSpec((tk, tn), lambda n, k: (k, n))
    shape = lambda rows: jax.ShapeDtypeStruct((rows, cols), jnp.float32)
    return pl.pallas_call(
        functools.partial(apply_kernel, n_rows, n_cols, grid[0] * grid[1]),
        out_shape=(shape(2 * m), shape(m)),
        grid=grid,
        in_specs=[pl.BlockSpec(memory_space=pltpu.VMEM), block, block],
        out_specs=[pl.BlockSpec((2 * m, tn), lambda n, k: (0, n)), pl.BlockSpec(memory_space=pltpu.VMEM)],
        scratch_shapes=[pltpu.VMEM((2 * m, rows), jnp.bfloat16), pltpu.VMEM((m, cols), jnp.float32)]
        + [pltpu.SemaphoreType.DMA((n_rows,)), pltpu.SemaphoreType.DMA((1,))],
        compiler_params=pltpu.CompilerParams(
            collective_id=collective_id, has_side_effects=True, dimension_semantics=("arbitrary", "arbitrary")
        ),
        name="apply_both",
    )(x_rows, a_matrix, b_matrix)


def gather_kernel(n_rows, n_cols, chunks, x_ref, o_ref, from_up, from_down, inward, row_send, up_recv, down_recv, send, recv):
    r, c = lax.axis_index("row"), lax.axis_index("col")
    ratio = n_cols // n_rows
    home, part = c // ratio, c % ratio
    width = x_ref.shape[1]
    step = width // chunks
    bits = n_cols.bit_length() - 1
    has_up, has_down = r < n_rows - 1, r > 0

    def bit(value, i):
        return value // 2**i % 2

    def flip(i):
        return c + 2**i * (1 - 2 * bit(c, i))

    barrier = pltpu.get_barrier_semaphore()
    for i in range(bits):
        greet(barrier, col=flip(i))
    meet(n_rows, bits)

    def lanes(ref, k):
        return ref.at[:, k * step : (k + 1) * step]

    def to_down(k, src):
        return remote(src, lanes(from_up, k), row_send.at[k], up_recv.at[k], row=r - 1)

    def to_up(k, src):
        return remote(src, lanes(from_down, k), row_send.at[k], down_recv.at[k], row=r + 1)

    def reduce(k):
        own = lanes(x_ref, k)

        @pl.when(r > home)
        def _():
            @pl.when(has_up)
            def _():
                to_down(k, own).wait_recv()
                lanes(inward, k)[...] = own[...] + lanes(from_up, k)[...]
                to_down(k, lanes(inward, k)).start()

            @pl.when(jnp.logical_not(has_up))
            def _():
                to_down(k, own).start()

        @pl.when(r < home)
        def _():
            @pl.when(has_down)
            def _():
                to_up(k, own).wait_recv()
                lanes(inward, k)[...] = own[...] + lanes(from_down, k)[...]
                to_up(k, lanes(inward, k)).start()

            @pl.when(jnp.logical_not(has_down))
            def _():
                to_up(k, own).start()

        @pl.when(r == home)
        def _():
            mine = o_ref.at[:, pl.ds(pl.multiple_of(part * width + k * step, 128), step)]

            @pl.when(has_up)
            def _():
                to_down(k, own).wait_recv()

            @pl.when(has_down)
            def _():
                to_up(k, own).wait_recv()

            @pl.when(has_up & has_down)
            def _():
                mine[...] = own[...] + (lanes(from_up, k)[...] + lanes(from_down, k)[...])

            @pl.when(jnp.logical_not(has_down))
            def _():
                mine[...] = own[...] + lanes(from_up, k)[...]

            @pl.when(jnp.logical_not(has_up))
            def _():
                mine[...] = own[...] + lanes(from_down, k)[...]

    def copies(p, k):
        apart = [(bit(c, i) + bit(r * ratio + p, i)) % 2 for i in range(bits)]
        top = [*range(bits - 1, 0, -1)]
        turn = k % len(top)
        order = [*top[turn:], *top[:turn], 0]
        spot = o_ref.at[:, p * width + k * step : p * width + (k + 1) * step]
        out = []
        for j, i in enumerate(order):
            later = sum(apart[x] for x in order[j:])
            out.append((later == 0, remote(spot, spot, send.at[p, k, j], recv.at[p, k], col=flip(i))))
        return out, sum(apart) > 0

    def broadcast(p, k, root):
        sends, inner = copies(p, k)

        @pl.when(jnp.logical_not(inner) if root else inner)
        def _():
            if not root:
                sends[0][1].wait_recv()
            for j, (condition, copy) in enumerate(sends):
                if root:
                    copy.start()
                elif j:

                    @pl.when(condition)
                    def _():
                        copy.start()

    for i in range(chunks):
        reduce(i)
        for p in range(ratio):
            broadcast(p, i, True)
    for i in range(chunks):
        for p in range(ratio):
            broadcast(p, i, False)
    for k in range(chunks):
        @pl.when(r > home)
        def _():
            to_down(k, lanes(x_ref, k)).wait_send()

        @pl.when(r < home)
        def _():
            to_up(k, lanes(x_ref, k)).wait_send()

        for p in range(ratio):
            for condition, copy in copies(p, k)[0]:

                @pl.when(condition)
                def _():
                    copy.wait_send()


def gather_sum(value, collective_id):
    n_rows, n_cols = lax.axis_size("row"), lax.axis_size("col")
    m, width = value.shape
    ratio = n_cols // n_rows
    chunks = min(4, width // 128)
    dma = pltpu.SemaphoreType.DMA
    return pl.pallas_call(
        functools.partial(gather_kernel, n_rows, n_cols, chunks),
        out_shape=jax.ShapeDtypeStruct((m, ratio * width), jnp.float32),
        in_specs=[pl.BlockSpec(memory_space=pltpu.VMEM)],
        out_specs=pl.BlockSpec(memory_space=pltpu.VMEM),
        scratch_shapes=[pltpu.VMEM((m, width), jnp.float32)] * 3
        + [dma((chunks,))] * 3
        + [dma((ratio, chunks, n_cols.bit_length() - 1)), dma((ratio, chunks))],
        compiler_params=pltpu.CompilerParams(collective_id=collective_id, has_side_effects=True),
        name="gather_sum",
    )(value)


def sum_kernel(n_rows, n_cols, over_rows, x_ref, o_ref, pair_buf, part, group_buf, row_buf, *sems):
    pair_send, pair_recv, group_send, group_recv, row_send, row_recv, all_send, all_recv, back_send, back_recv = sems
    r, c = lax.axis_index("row"), lax.axis_index("col")
    half = n_cols // 2
    g, h = c // 2, c % 2
    partner = 2 * g + 1 - h
    flat = len(x_ref.shape) == 2
    step = x_ref.shape[-1] // n_cols

    def piece(ref, index):
        return ref.at[:, pl.ds(pl.multiple_of(index * step, 128), step)] if flat else ref.at[index]

    barrier = pltpu.get_barrier_semaphore()
    greet(barrier, col=partner)
    for d in range(1, half):
        greet(barrier, col=2 * ((g + d) % half) + h)
    if over_rows:
        for e in range(1, n_rows):
            greet(barrier, row=(r + e) % n_rows)
    pl.semaphore_wait(barrier, half + (n_rows - 1 if over_rows else 0))

    order = [*range(1, half), 0]
    started = []
    pair = {}
    for d in order:
        j = (g + d) % half
        pair[d] = remote(piece(x_ref, (1 - h) * half + j), pair_buf.at[d], pair_send.at[d], pair_recv.at[d], col=partner)
        pair[d].start()
        started.append(pair[d])
    group = {}
    for d in order:
        j = (g + d) % half
        pair[d].wait_recv()
        value = piece(x_ref, h * half + j)[...] + pair_buf[d]
        if d:
            part[d] = value
            group[d] = remote(part.at[d], group_buf.at[d], group_send.at[d], group_recv.at[d], col=2 * j + h)
            group[d].start()
            started.append(group[d])
    for d in range(1, half):
        group[d].wait_recv()
        value = value + group_buf[d]
    if over_rows:
        row_buf[r] = value
        rows = []
        for e in range(1, n_rows):
            rows.append(remote(row_buf.at[r], row_buf.at[r], row_send.at[e], row_recv.at[e], row=(r + e) % n_rows))
            rows[-1].start()
        started.extend(rows)
        for e in range(1, n_rows):
            source = (r - e + n_rows) % n_rows
            remote(row_buf.at[source], row_buf.at[source], row_send.at[e], row_recv.at[e], row=source).wait_recv()
        value = row_buf[0]
        for e in range(1, n_rows):
            value = value + row_buf[e]
    mine = piece(o_ref, h * half + g)
    mine[...] = value
    for d in range(1, half):
        copy = remote(mine, mine, all_send.at[d], all_recv.at[d], col=2 * ((g + d) % half) + h)
        copy.start()
        started.append(copy)
    for d in range(half):
        j = (g - d + half) % half
        got = piece(o_ref, h * half + j)
        if d:
            remote(got, got, all_send.at[d], all_recv.at[d], col=2 * j + h).wait_recv()
        copy = remote(got, got, back_send.at[d], back_recv.at[d], col=partner)
        copy.start()
        started.append(copy)
    for d in range(half):
        got = piece(o_ref, (1 - h) * half + (g - d + half) % half)
        remote(got, got, back_send.at[d], back_recv.at[d], col=partner).wait_recv()
    for copy in started:
        copy.wait_send()


def sum_over(value, collective_id, over_rows):
    n_rows, n_cols = lax.axis_size("row"), lax.axis_size("col")
    half = n_cols // 2
    shape = (value.shape[0], value.shape[1] // n_cols) if value.ndim == 2 else value.shape[1:]
    dma = pltpu.SemaphoreType.DMA
    return pl.pallas_call(
        functools.partial(sum_kernel, n_rows, n_cols, over_rows),
        out_shape=jax.ShapeDtypeStruct(value.shape, jnp.float32),
        in_specs=[pl.BlockSpec(memory_space=pltpu.VMEM)],
        out_specs=pl.BlockSpec(memory_space=pltpu.VMEM),
        scratch_shapes=[pltpu.VMEM((half, *shape), jnp.float32)] * 3
        + [pltpu.VMEM((n_rows if over_rows else 1, *shape), jnp.float32)]
        + [dma((half,))] * 4
        + [dma((n_rows,))] * 2
        + [dma((half,))] * 4,
        compiler_params=pltpu.CompilerParams(collective_id=collective_id, has_side_effects=True),
        name="sum_over",
    )(value)


def total(value, collective_id):
    n_cols = lax.axis_size("col")
    rows, cols = value.shape
    return sum_over(value.reshape(n_cols, rows // n_cols, cols), collective_id, True)


PANEL = 8


def block_inverse(block):
    size = block.shape[0]
    shape = (size, 2 * size)
    rows = lax.broadcasted_iota(jnp.int32, shape, 0)
    cols = lax.broadcasted_iota(jnp.int32, shape, 1)
    ident = jnp.where(rows == cols, 1.0, 0.0)[:, :size]
    work = jnp.concatenate([block, ident], axis=1)
    for start in range(0, size, PANEL):
        spread = [jnp.broadcast_to(work[:, start + i : start + i + 1], shape) for i in range(PANEL)]
        for i in range(PANEL):
            j = start + i
            column = spread[i]
            factor = jnp.where(rows > j, column, 0.0) * (1.0 / column[j : j + 1])
            for later in range(i + 1, PANEL):
                spread[later] = spread[later] - factor * column[start + later : start + later + 1]
            work = work - factor * work[j : j + 1]
    diag = jnp.sum(jnp.where(rows == cols, work, 0.0), axis=1, keepdims=True)
    return work[:, size:] / jnp.sqrt(diag)


def mm_split(left, right):
    left_high, left_low = halves(left)
    right_high, right_low = halves(right)
    return dot(left_high, right_high) + (dot(left_high, right_low) + dot(left_low, right_high))


def solve(order, k, ga, gb, linv_ref, sym_ref):
    n = ga.shape[0]
    sym_ref[...] = gb
    nb = n // k
    cut = lambda ref, i, j: ref[i * k : (i + 1) * k, j * k : (j + 1) * k]
    linv_ref[...] = jnp.zeros((n, n), jnp.float32)
    low, inv = {}, {}
    for j in range(nb):
        for i in range(j, nb):
            rest = cut(sym_ref, i, j)
            for m in range(j):
                rest = rest - mm(low[i, m], low[j, m], 1, 1)
            if i == j:
                inv[j, j] = block_inverse(rest)
            else:
                low[i, j] = mm(rest, inv[j, j], 1, 1)
    for j in range(nb):
        for i in range(j + 1, nb):
            total = mm(low[i, j], inv[j, j])
            for m in range(j + 1, i):
                total = total + mm(low[i, m], inv[m, j])
            inv[i, j] = -mm(inv[i, i], total)
    for (i, j), value in inv.items():
        linv_ref[i * k : (i + 1) * k, j * k : (j + 1) * k] = value
    linv = linv_ref[...]
    linv_t = linv.T
    middle = mm(mm(linv, ga), linv_t)
    middle = 0.5 * (middle + middle.T)
    rows = lax.broadcasted_iota(jnp.int32, (n, n), 0)
    cols = lax.broadcasted_iota(jnp.int32, (n, n), 1)
    ident = jnp.where(rows == cols, 1.0, 0.0)
    shift = jnp.sum(middle * ident) / n
    centred = middle - shift * ident
    sign_est = centred / jnp.sqrt(jnp.full((1, 1), jnp.sum(centred * centred) + 1e-06))
    for turn in range(NS_STEPS):
        sign_est = 1.5 * sign_est - 0.5 * mm_split(sign_est, mm_split(sign_est, sign_est))
    filtered = (0.5 * (ident - sign_est))[:, :k]
    coords = mm(linv_t, filtered) * math.sqrt(order)
    reduced = mm(filtered.T, mm(middle, filtered))
    return coords, mm(coords, reduced)


def outer_rows(value, k):
    return jnp.where((lax.broadcasted_iota(jnp.int32, value.shape, 0) >= k), value, 0.0)


def first_kernel(order, grams_ref, w_ref, mix_ref, wa_ref, wb_ref, linv_ref, sym_ref):
    n, k = w_ref.shape[0], mix_ref.shape[1]
    grams = grams_ref[...].reshape(2 * n, n)
    ga, gb = grams[:n], grams[n:]
    ga, gb = 0.5 * (ga + ga.T), 0.5 * (gb + gb.T)
    coords, reduced = solve(order, k, ga, gb, linv_ref, sym_ref)
    mix_ref[:n] = coords
    mix_ref[n:] = -reduced
    w_ref[:, :k] = coords
    w_ref[:, k:] = outer_rows(coords, k)
    w = w_ref[...]
    w_t = w.T
    wa_ref[...] = mm(w_t, mm(ga, w))
    wb_ref[...] = mm(w_t, mm(sym_ref[...], w))


def second_kernel(order, wa_ref, wb_ref, w_ref, grams_ref, wide_ref, inner_ref, mix_ref, mix_in_ref, linv_ref, sym_ref, ga_ref, c_ref):
    n, k = w_ref.shape[0], mix_ref.shape[1]
    grams = grams_ref[...].reshape(2 * k, n + k)
    w = w_ref[...]
    for at, kept in enumerate((wa_ref, wb_ref)):
        fresh = grams[at * k : (at + 1) * k]
        ends = mm(fresh[:, :n], w)
        middle = fresh[:, n:]
        full = ga_ref.at[at]
        full[:k, :k] = kept[:k, :k]
        full[:k, 2 * k :] = kept[:k, k:]
        full[2 * k :, :k] = kept[k:, :k]
        full[2 * k :, 2 * k :] = kept[k:, k:]
        full[k : 2 * k, :k] = ends[:, :k]
        full[k : 2 * k, 2 * k :] = ends[:, k:]
        full[k : 2 * k, k : 2 * k] = middle
        full[:k, k : 2 * k] = ends[:, :k].T
        full[2 * k :, k : 2 * k] = ends[:, k:].T
    ga, gb = ga_ref[0], ga_ref[1]
    ga, gb = 0.5 * (ga + ga.T), 0.5 * (gb + gb.T)
    coords, reduced = solve(order, k, ga, gb, linv_ref, sym_ref)
    c_ref[:, :k] = coords
    c_ref[:, k : 2 * k] = outer_rows(coords, k)
    c_ref[:, 2 * k :] = reduced
    ends = mm(w[:, :k], c_ref[:k]) + mm(w[:, k:], c_ref[2 * k :])
    wide_ref[...] = ends[:, : 2 * k]
    inner_ref[...] = c_ref[k : 2 * k, : 2 * k]
    mix_ref[:n] = ends[:, :k]
    mix_ref[n:] = -ends[:, 2 * k :]
    mix_in_ref[:k] = c_ref[k : 2 * k, :k]
    mix_in_ref[k:] = -c_ref[k : 2 * k, 2 * k :]


def in_vmem(kernel, shapes, scratch, name, *args):
    return pl.pallas_call(
        kernel,
        out_shape=tuple(jax.ShapeDtypeStruct(dims, jnp.float32) for dims in shapes),
        in_specs=[pl.BlockSpec(memory_space=pltpu.VMEM)] * len(args),
        out_specs=[pl.BlockSpec(memory_space=pltpu.VMEM)] * len(shapes),
        scratch_shapes=[pltpu.VMEM(dims, jnp.float32) for dims in scratch],
        name=name,
    )(*args)


def first_ritz(order, k, grams):
    n = grams.shape[-1]
    shapes = ((n, 2 * k), (2 * n, k), (2 * k, 2 * k), (2 * k, 2 * k))
    return in_vmem(functools.partial(first_kernel, order), shapes, [(n, n)] * 2, "first_ritz", grams)


def second_ritz(order, k, kept_a, kept_b, w, grams):
    n = w.shape[0]
    shapes = ((n, 2 * k), (k, 2 * k), (2 * n, k), (2 * k, k))
    scratch = [(n, n)] * 2 + [(2, n, n), (n, 3 * k)]
    return in_vmem(functools.partial(second_kernel, order), shapes, scratch, "second_ritz", kept_a, kept_b, w, grams)


def local(order, a_matrix, b_matrix, x_block, r_block, p_block):
    k = x_block.shape[1]
    panel = jnp.concatenate([x_block.T, r_block.T, p_block.T], axis=0)
    prods, tile = apply_both(panel, a_matrix, b_matrix, 0)
    grams = total(mm(prods, tile, 1, 1, HIGH), 1)
    w, mix, kept_a, kept_b = first_ritz(order, k, grams)
    resid = gather_sum(mm(mix, prods, 0, 0, HIGH), 2)
    fresh, resid_tile = apply_both(resid, a_matrix, b_matrix, 3)
    ends = mm(fresh, tile, 1, 1, HIGH)
    mirror = mm(resid_tile, prods, 1, 1, HIGH)
    mirror = jnp.concatenate([mirror[:, : 3 * k], mirror[:, 3 * k :]], axis=0)
    grams = total(jnp.concatenate([0.5 * (ends + mirror), mm(fresh, resid_tile, 1, 1, HIGH)], axis=1), 4)
    wide, inner, mix, mix_in = second_ritz(order, k, kept_a, kept_b, w, grams)
    last = gather_sum(mm(mix, prods, 0, 0, HIGH) + mm(mix_in, fresh, 0, 0, HIGH), 5)
    both = mm(wide, panel, 0, 0, HIGH) + mm(inner, resid, 0, 0, HIGH)
    return (both[:k].T, last.T, both[k:].T)


def solution(mesh):
    def whole(a_matrix, b_matrix, x_block, r_block, p_block):
        return jax.shard_map(
            functools.partial(local, a_matrix.shape[0]),
            mesh=mesh,
            in_specs=(P("row", "col"), P("row", "col"), P("row", None), P("row", None), P("row", None)),
            out_specs=(P("row", None), P("row", None), P("row", None)),
            check_vma=False,
        )(a_matrix, b_matrix, x_block, r_block, p_block)

    return whole
```
